32 devices in a mesh: lat: 4 (over z), lon: 4 (over x, core), lev: 2 (over y).
Axes of the slice: x: 2, y: 2, z: 4, core: 2. Of those that a mesh axis runs over, the one named last changes fastest.
Arguments:
- field_now: float32 [16, 256, 128, 128], P('lat', 'lon', 'lev'), may hold values from 0.2 to 1.8
- earlier: float32 [16, 256, 128, 128], P('lat', 'lon', 'lev'), may hold values from 0.2 to 1.8
- speed_square: float32 [16, 256, 128, 128], P('lat', 'lon', 'lev'), may hold values from 0.05 to 0.3
Outputs:
- field_now_end: float32 [16, 256, 128, 128], P('lat', 'lon', 'lev')
The draws below stay inside these ranges and needn't reach their ends.
All inputs are finite; a program needn't handle non-finite values.
Results may differ from the reference program's by a relative error of at most 0.00002.
Values sent between devices are 32-bit elements; how exact they have to be, the bound alone decides.
No kernel may reach another device: no remote copies, remote signals or barrier semaphores. Data moves between devices by JAX's collectives and lax.ppermute only.
A program may use at most 320 MiB of HBM per device.

```python
import jax
import jax.numpy as jnp
from jax import lax

GRID_J = 16
GRID_I = 256
GRID_K = 128
MEMBERS = 128
STEPS = 4


def block_levels(stream_key, shape, cuts, least, largest):
    def one(axis_at, blocks):
        draws = jax.random.uniform(jax.random.fold_in(jax.random.fold_in(stream_key, 6), axis_at), (blocks,), jnp.float32, least / len(cuts), largest / len(cuts))
        return jnp.repeat(jnp.exp(draws), shape[axis_at] // blocks).reshape((-1,) + (1,) * (len(shape) - axis_at - 1))

    gain = one(*cuts[0])
    for cut in cuts[1:]:
        gain = gain * one(*cut)
    return gain


def setup_inputs(seed: int = 0) -> dict:
    arg_keys = jax.random.split(jax.random.key(seed), 4)
    field_now = jnp.clip(0.2 + 1.5999999 * jax.random.uniform(arg_keys[0], (GRID_J, GRID_I, GRID_K, MEMBERS), jnp.float32) ** block_levels(arg_keys[0], (GRID_J, GRID_I, GRID_K, MEMBERS), ((0, 4), (1, 4), (2, 2)), -0.2, 0.2), 0.2, 1.8)
    earlier = jnp.clip(0.2 + 1.5999999 * jax.random.uniform(arg_keys[1], (GRID_J, GRID_I, GRID_K, MEMBERS), jnp.float32) ** block_levels(arg_keys[1], (GRID_J, GRID_I, GRID_K, MEMBERS), ((0, 4), (1, 4), (2, 2)), -0.2, 0.2), 0.2, 1.8)
    speed_square = jnp.clip(0.05 + 0.25 * jax.random.uniform(arg_keys[2], (GRID_J, GRID_I, GRID_K, MEMBERS), jnp.float32) ** block_levels(arg_keys[2], (GRID_J, GRID_I, GRID_K, MEMBERS), ((0, 4), (1, 4), (2, 2)), -0.2, 0.2), 0.05, 0.3)
    return {"field_now": field_now, "earlier": earlier, "speed_square": speed_square}


def without_rim(values, dims):
    for dim in dims:
        values = lax.slice_in_dim(values, 1, values.shape[dim] - 1, axis=dim)
    return values


def shifted_cells(values, dim, start, dims):
    others = [other for other in dims if other != dim]
    values = without_rim(values, others)
    return lax.slice_in_dim(values, start, start + values.shape[dim] - 2, axis=dim)


def march_step(padded, before, speed_square):
    middle = without_rim(padded, (0, 1, 2))
    lower = [shifted_cells(padded, dim, 0, (0, 1, 2)) for dim in (0, 1, 2)]
    upper = [shifted_cells(padded, dim, 2, (0, 1, 2)) for dim in (0, 1, 2)]
    spread = lower[0] + upper[0] + lower[1] + upper[1] + lower[2] + upper[2] - 6.0 * middle
    return 2.0 * middle - before + speed_square * spread


def reference(field_now, earlier, speed_square):
    for step in range(STEPS):
        later = march_step(jnp.pad(field_now, ((1, 1), (1, 1), (1, 1), (0, 0)), mode="constant"), earlier, speed_square)
        earlier, field_now = field_now, later
    return field_now
```

```python
import functools

import jax
import jax.numpy as jnp
from jax import lax
from jax.experimental import pallas as pl
from jax.experimental.pallas import tpu as pltpu
from jax.sharding import PartitionSpec as P

STEPS = 4
CHUNKS = 2
ROWS = 8


def sent(value, axis, up):
    peers = lax.axis_size(axis)
    pairs = [(i, i + 1) for i in range(peers - 1)]
    if not up:
        pairs = [(j, i) for i, j in pairs]
    return lax.ppermute(value, axis, pairs)


def piece_body(plane0, row0, rows, total, has_out, has_edge, *refs):
    here, row_lo, row_hi, lower, upper, lon_lo, lon_hi, lev_lo, lev_hi, speed, before = refs[:11]
    outs = refs[11 + has_out:]
    depth = here.shape[2]
    at = row0 + pl.program_id(1) * rows
    first = at == 0
    last = at + rows == total
    level = lax.broadcasted_iota(jnp.int32, (depth, here.shape[3]), 0)
    for r in range(rows):
        mid = here[0, r]
        if r == 0:
            left = jnp.where(first, lon_lo[0], row_lo[0, 0])
        else:
            left = here[0, r - 1]
        if r == rows - 1:
            right = jnp.where(last, lon_hi[0], row_hi[0, 0])
        else:
            right = here[0, r + 1]
        below = jnp.where(level == 0, lev_lo[0, r:r + 1], pltpu.roll(mid, 1, 0))
        above = jnp.where(level == depth - 1, lev_hi[0, r:r + 1], pltpu.roll(mid, depth - 1, 0))
        spread = lower[0, r] + upper[0, r] + left + right + below + above - 6.0 * mid
        later = 2.0 * mid - before[0, r] + speed[0, r] * spread
        for out in outs:
            out[0, r] = later


def piece(field, before, speed, out, halos, faces, plane0, planes, row0, length, edge):
    lon_lo, lon_hi, lev_lo, lev_hi = faces
    J, I, K, M = field.shape
    rows = ROWS
    base = row0 // rows

    def cells(shift):
        return pl.BlockSpec((1, rows, K, M), lambda p, b: (plane0 + p + shift, base + b, 0, 0))

    halo = pl.BlockSpec((1, rows, K, M), lambda p, b: (p, b, 0, 0))
    one = pl.BlockSpec((1, 1, K, M), lambda p, b: (plane0 + p, jnp.maximum((base + b) * rows - 1, 0), 0, 0))
    two = pl.BlockSpec((1, 1, K, M), lambda p, b: (plane0 + p, jnp.minimum((base + b + 1) * rows, I - 1), 0, 0))
    lon = pl.BlockSpec((1, K, M), lambda p, b: (plane0 + p, 0, 0))
    lev = pl.BlockSpec((1, rows, M), lambda p, b: (plane0 + p, base + b, 0))
    lower, upper = halos
    operands = [field, field, field,
                field if lower is None else lower, field if upper is None else upper,
                lon_lo, lon_hi, lev_lo, lev_hi, speed, before]
    specs = [cells(0), one, two,
             cells(-1) if lower is None else halo, cells(1) if upper is None else halo,
             lon, lon, lev, lev, cells(0), cells(0)]
    aliases = {}
    if out is not None:
        aliases = {len(operands): 0}
        operands.append(out)
        specs.append(pl.BlockSpec(memory_space=pl.ANY))
    shapes = [jax.ShapeDtypeStruct(field.shape, field.dtype)]
    out_specs = [cells(0)]
    if edge:
        shapes.append(jax.ShapeDtypeStruct((1, length, K, M), field.dtype))
        out_specs.append(halo)
    count = planes * length * K * M
    results = pl.pallas_call(
        functools.partial(piece_body, plane0, row0, rows, I, int(out is not None), edge),
        grid=(planes, length // rows),
        in_specs=specs,
        out_specs=out_specs,
        out_shape=shapes,
        input_output_aliases=aliases,
        cost_estimate=pl.CostEstimate(flops=12 * count, bytes_accessed=24 * count, transcendentals=0),
        name=f"piece_{plane0}_{row0}",
    )(*operands)
    return results if edge else (results[0], None)


def side_faces(field):
    J, I, K, M = field.shape
    rows = [lax.slice_in_dim(field, at, at + 1, axis=1).reshape(J, K, M) for at in (0, I - 1)]
    levels = [lax.slice_in_dim(field, at, at + 1, axis=2).reshape(J, I, M) for at in (0, K - 1)]
    return (sent(rows[1], "lon", True), sent(rows[0], "lon", False),
            sent(levels[1], "lev", True), sent(levels[0], "lev", False))


def local(field_now, earlier, speed_square):
    J, I, K, M = field_now.shape
    length = I // CHUNKS
    starts = [c * length for c in range(CHUNKS)]
    lows, highs = [], []
    for at in starts:
        top = lax.slice(field_now, (J - 1, at, 0, 0), (J, at + length, K, M))
        bottom = lax.slice(field_now, (0, at, 0, 0), (1, at + length, K, M))
        lows.append(sent(top, "lat", True))
        highs.append(sent(bottom, "lat", False))
    for step in range(STEPS):
        final = step == STEPS - 1
        faces = side_faces(field_now)
        later = None
        next_lows, next_highs = [], []
        run = functools.partial(piece, field_now, earlier, speed_square)
        for c, at in enumerate(starts):
            later, bottom = run(later, (lows[c], None), faces, 0, 1, at, length, not final)
            if not final:
                next_highs.append(sent(bottom, "lat", False))
            later, top = run(later, (None, highs[c]), faces, J - 1, 1, at, length, not final)
            if not final:
                next_lows.append(sent(top, "lat", True))
            if c == 0 and J > 2:
                later, _ = run(later, (None, None), faces, 1, J - 2, 0, I, False)
        lows, highs = next_lows, next_highs
        earlier, field_now = field_now, later
    return field_now


def solution(mesh):
    spec = P("lat", "lon", "lev", None)
    return jax.shard_map(
        local,
        mesh=mesh,
        in_specs=(spec, spec, spec),
        out_specs=spec,
        check_vma=False,
    )
```

```python
import functools

import jax
import jax.numpy as jnp
from jax import lax
from jax.experimental import pallas as pl
from jax.experimental.pallas import tpu as pltpu
from jax.sharding import PartitionSpec as P

STEPS = 4
CHUNKS = 2
LIMIT = 2 * 1024 * 1024


ANY = pl.BlockSpec(memory_space=pl.ANY)
VMEM = pl.BlockSpec(memory_space=pltpu.VMEM)


def sent(value, axis, up):
    peers = lax.axis_size(axis)
    pairs = [(i, i + 1) for i in range(peers - 1)]
    if not up:
        pairs = [(j, i) for i, j in pairs]
    return lax.ppermute(value, axis, pairs)


def held(value):
    return pltpu.with_memory_space_constraint(value, pltpu.VMEM)


def call(body, operands, in_specs, out_shape, out_specs, cost, name, aliases=None, scratch=()):
    return pl.pallas_call(
        body,
        in_specs=in_specs,
        out_specs=out_specs,
        out_shape=out_shape,
        scratch_shapes=list(scratch),
        input_output_aliases=aliases or {},
        cost_estimate=pl.CostEstimate(flops=12 * cost, bytes_accessed=4 * cost, transcendentals=0),
        compiler_params=pltpu.CompilerParams(vmem_limit_bytes=LIMIT),
        name=name,
    )(*operands)


def face_shapes(shape, dtype):
    J, I, K, M = shape
    return [pltpu.VMEM((J, K, M), dtype)] * 2 + [pltpu.VMEM((J, I, M), dtype)] * 2


def write_faces(cells, faces):
    J, I, K, M = cells.shape
    for p in range(J):
        faces[0][p] = cells[p, 0]
        faces[1][p] = cells[p, I - 1]

        @pl.loop(0, I // 8)
        def _(b):
            for r in range(8):
                at = b * 8 + r
                faces[2][p, pl.ds(at, 1), :] = cells[p, at, 0:1, :]
                faces[3][p, pl.ds(at, 1), :] = cells[p, at, K - 1:K, :]


def copied(pairs, sems):
    copies = [pltpu.make_async_copy(a, b, sems.at[n]) for n, (a, b) in enumerate(pairs)]
    for copy in copies:
        copy.start()
    for copy in copies:
        copy.wait()


def stage_body(row0, length, whole, field, *refs):
    J = field.shape[0]
    rows = pl.ds(row0, length)
    low, high = refs[:2]
    pairs = [(field.at[pl.ds(0, 1), rows], low), (field.at[pl.ds(J - 1, 1), rows], high)]
    if whole:
        pairs.append((field, refs[2]))
    copied(pairs, refs[-1])
    if whole:
        write_faces(refs[2], refs[3:7])


def load_body(before_in, speed_in, before, speed, sems):
    copied([(before_in, before), (speed_in, speed)], sems)


def cell_row(refs, p, r, left, right, lower, upper):
    here, before, speed, lev_lo, lev_hi, out = refs
    mid = here[p, r]
    depth = mid.shape[0]
    level = lax.broadcasted_iota(jnp.int32, mid.shape, 0)
    below = jnp.where(level == 0, lev_lo[p, pl.ds(r, 1), :], pltpu.roll(mid, 1, 0))
    above = jnp.where(level == depth - 1, lev_hi[p, pl.ds(r, 1), :], pltpu.roll(mid, depth - 1, 0))
    spread = lower + upper + left + right + below + above - 6.0 * mid
    later = 2.0 * mid - before[p, r] + speed[p, r] * spread
    out[p, r] = later
    return later


def edge_body(row0, length, final, last, *refs):
    here, before, speed, lon_lo, lon_hi, lev_lo, lev_hi, from_low, from_high = refs[:9]
    refs = refs[9:]
    result = None
    if final:
        refs, sems, result = refs[1:-1], refs[-1], refs[2]
    out = refs[0]
    sends = () if final else refs[1:3]
    J, I, K, M = here.shape
    shared = (here, before, speed, lev_lo, lev_hi, out)

    def both(r, left_of, right_of):
        value = cell_row(shared, 0, r, left_of(0), right_of(0), from_low[0, r - row0], here[1, r])
        if not final:
            sends[0][0, r - row0] = value
        value = cell_row(shared, J - 1, r, left_of(J - 1), right_of(J - 1), here[J - 2, r], from_high[0, r - row0])
        if not final:
            sends[1][0, r - row0] = value

    low, high = max(row0, 1), min(row0 + length, I - 1)
    if row0 == 0:
        both(0, lambda p: lon_lo[p], lambda p: here[p, 1])

    @pl.loop(low, high)
    def _(r):
        both(r, lambda p: here[p, r - 1], lambda p: here[p, r + 1])

    if row0 + length == I:
        both(I - 1, lambda p: here[p, I - 2], lambda p: lon_hi[p])
    if final:
        rows = pl.ds(row0, length)
        copied([(out.at[p, rows], result.at[p, rows]) for p in (0, J - 1)], sems)
    elif last:
        write_faces(out, refs[3:7])


def inner_body(final, *refs):
    here, before, speed, lon_lo, lon_hi, lev_lo, lev_hi = refs[:7]
    refs = refs[7:]
    out = refs[0]
    J, I, K, M = here.shape
    shared = (here, before, speed, lev_lo, lev_hi, out)

    @pl.loop(1, J - 1)
    def _(p):
        cell_row(shared, p, 0, lon_lo[p], here[p, 1], here[p - 1, 0], here[p + 1, 0])

        @pl.loop(1, I - 1)
        def _(r):
            cell_row(shared, p, r, here[p, r - 1], here[p, r + 1], here[p - 1, r], here[p + 1, r])

        cell_row(shared, p, I - 1, here[p, I - 2], lon_hi[p], here[p - 1, I - 1], here[p + 1, I - 1])

    if final:
        inner = pl.ds(1, J - 2)
        copied([(out.at[inner], refs[1].at[inner])], refs[2])


def local(field_now, earlier, speed_square):
    J, I, K, M = shape = field_now.shape
    dtype = field_now.dtype
    length = I // CHUNKS
    starts = [c * length for c in range(CHUNKS)]
    lat_chunk = pltpu.VMEM((1, length, K, M), dtype)
    block = pltpu.VMEM(shape, dtype)
    lev_pair = lax.axis_size("lev") == 2
    lev_at = lax.axis_index("lev")

    def exchange(faces):
        first, final, under, over = faces
        lon_lo, lon_hi = sent(final, "lon", True), sent(first, "lon", False)
        lev_lo, lev_hi = sent(over, "lev", True), sent(under, "lev", False)
        return [held(x) for x in (lon_lo, lon_hi, lev_lo, lev_hi)]

    lows, highs = [], []
    for c, at in enumerate(starts):
        whole = c == CHUNKS - 1
        shapes = [lat_chunk] * 2 + ([block] + face_shapes(shape, dtype) if whole else [])
        got = call(functools.partial(stage_body, at, length, whole), [field_now], [ANY], shapes,
                   [VMEM] * len(shapes), length * K * M, f"stage_{at}",
                   scratch=[pltpu.SemaphoreType.DMA((3,))])
        highs.append(sent(got[0], "lat", False))
        lows.append(sent(got[1], "lat", True))
    field, faces = got[2], exchange(got[3:7])
    before, speed = call(load_body, [earlier, speed_square], [ANY] * 2, [block] * 2, [VMEM] * 2,
                         J * I * K * M, "load", scratch=[pltpu.SemaphoreType.DMA((2,))])
    result = None
    for step in range(STEPS):
        final = step == STEPS - 1
        next_lows, next_highs = [], []
        for c, at in enumerate(starts):
            last = c == CHUNKS - 1
            operands = [held(field), held(before), held(speed), *faces, held(lows[c]), held(highs[c])]
            in_specs = [VMEM] * 9
            aliases = {1: 0}
            shapes, out_specs, scratch = [block], [VMEM], []
            if final:
                operands.append(result)
                in_specs.append(ANY)
                aliases[9] = 1
                shapes.append(jax.ShapeDtypeStruct(shape, dtype))
                out_specs.append(ANY)
                scratch = [pltpu.SemaphoreType.DMA((2,))]
                if c == 0:
                    operands[1], result = call(
                        functools.partial(inner_body, True), operands[:7], [VMEM] * 7, shapes, out_specs,
                        (J - 2) * I * K * M, f"inner_{step}", {1: 0}, [pltpu.SemaphoreType.DMA((1,))])
                    operands[1], operands[9] = held(operands[1]), result
            else:
                shapes += [lat_chunk] * 2
                if last:
                    shapes += face_shapes(shape, dtype)
                out_specs = [VMEM] * len(shapes)
            got = call(functools.partial(edge_body, at, length, final, last), operands, in_specs, shapes,
                       out_specs, 2 * length * K * M, f"edge_{step}_{at}", aliases, scratch)
            before = got[0]
            if final:
                result = got[1]
                continue
            next_highs.append(sent(got[1], "lat", False))
            next_lows.append(sent(got[2], "lat", True))
            if last:
                next_faces = exchange(got[3:7])
            if c == 0 and J > 2:
                operands[1] = held(before)
                before, = call(functools.partial(inner_body, False), operands[:7], [VMEM] * 7, [block], [VMEM],
                               (J - 2) * I * K * M, f"inner_{step}", {1: 0})
        if not final:
            lows, highs, faces = next_lows, next_highs, next_faces
            before, field = field, before
    return result


def solution(mesh):
    spec = P("lat", "lon", "lev", None)
    return jax.shard_map(
        local,
        mesh=mesh,
        in_specs=(spec, spec, spec),
        out_specs=spec,
        check_vma=False,
    )
```

```python
import functools

import jax
import jax.numpy as jnp
from jax import lax
from jax.experimental import pallas as pl
from jax.experimental.pallas import tpu as pltpu
from jax.sharding import PartitionSpec as P

STEPS = 4
BLOCK = 8
LIMIT = 2 * 1024 * 1024


ANY = pl.BlockSpec(memory_space=pl.ANY)
VMEM = pl.BlockSpec(memory_space=pltpu.VMEM)


def sent(value, axis, up):
    peers = lax.axis_size(axis)
    pairs = [(i, i + 1) for i in range(peers - 1)]
    if not up:
        pairs = [(j, i) for i, j in pairs]
    return lax.ppermute(value, axis, pairs)


def held(value):
    return pltpu.with_memory_space_constraint(value, pltpu.VMEM)


def far(value):
    return pltpu.with_memory_space_constraint(value, pltpu.HBM)


def call(body, operands, in_specs, out_shape, out_specs, cost, name, aliases=None, scratch=()):
    return pl.pallas_call(
        body,
        in_specs=in_specs,
        out_specs=out_specs,
        out_shape=out_shape,
        scratch_shapes=list(scratch),
        input_output_aliases=aliases or {},
        cost_estimate=pl.CostEstimate(flops=12 * cost, bytes_accessed=4 * cost, transcendentals=0),
        compiler_params=pltpu.CompilerParams(vmem_limit_bytes=LIMIT),
        name=name,
    )(*operands)


def face_shapes(shape, dtype):
    J, I, K, M = shape
    return [pltpu.VMEM((J, K, M), dtype)] * 2 + [pltpu.VMEM((J, I, M), dtype)] * 2


def write_faces(cells, faces):
    J, I, K, M = cells.shape
    for p in range(J):
        faces[0][p] = cells[p, 0]
        faces[1][p] = cells[p, I - 1]

        @pl.loop(0, I // 8)
        def _(b):
            for r in range(8):
                at = b * 8 + r
                faces[2][p, pl.ds(at, 1), :] = cells[p, at, 0:1, :]
                faces[3][p, pl.ds(at, 1), :] = cells[p, at, K - 1:K, :]


def copied(pairs, sems):
    copies = [pltpu.make_async_copy(a, b, sems.at[n]) for n, (a, b) in enumerate(pairs)]
    for copy in copies:
        copy.start()
    for copy in copies:
        copy.wait()


def stage_body(row0, length, whole, field, *refs):
    J = field.shape[0]
    rows = pl.ds(row0, length)
    low, high = refs[:2]
    pairs = [(field.at[pl.ds(0, 1), rows], low), (field.at[pl.ds(J - 1, 1), rows], high)]
    if whole:
        pairs.append((field, refs[2]))
    copied(pairs, refs[-1])
    if whole:
        write_faces(refs[2], refs[3:7])


def load_body(before_in, speed_in, before, speed, sems):
    copied([(before_in, before), (speed_in, speed)], sems)


def cell_row(refs, p, r, left, right, lower, upper):
    here, before, speed, lev_lo, lev_hi, out = refs
    mid = here[p, r]
    depth = mid.shape[0]
    level = lax.broadcasted_iota(jnp.int32, mid.shape, 0)
    below = jnp.where(level == 0, lev_lo[p, pl.ds(r, 1), :], pltpu.roll(mid, 1, 0))
    above = jnp.where(level == depth - 1, lev_hi[p, pl.ds(r, 1), :], pltpu.roll(mid, depth - 1, 0))
    spread = lower + upper + left + right + below + above - 6.0 * mid
    later = 2.0 * mid - before[p, r] + speed[p, r] * spread
    out[p, r] = later
    return later


def edge_body(row0, length, last, *refs):
    here, before, speed, lon_lo, lon_hi, lev_lo, lev_hi, from_low, from_high = refs[:9]
    out, send_low, send_high = refs[9:12]
    J, I, K, M = here.shape
    shared = (here, before, speed, lev_lo, lev_hi, out)

    def both(r, left_of, right_of):
        at = r - row0
        send_low[0, at] = cell_row(shared, 0, r, left_of(0), right_of(0), from_low[0, at], here[1, r])
        send_high[0, at] = cell_row(
            shared, J - 1, r, left_of(J - 1), right_of(J - 1), here[J - 2, r], from_high[0, at])

    if row0 == 0:
        both(0, lambda p: lon_lo[p], lambda p: here[p, 1])

    @pl.loop(max(row0, 1), min(row0 + length, I - 1))
    def _(r):
        both(r, lambda p: here[p, r - 1], lambda p: here[p, r + 1])

    if row0 + length == I:
        both(I - 1, lambda p: here[p, I - 2], lambda p: lon_hi[p])
    if last:
        write_faces(out, refs[12:16])


def final_body(row0, length, low, *refs):
    here, before, speed, lon_lo, lon_hi, lev_lo, lev_hi, halo = refs[:8]
    out, result, sems = refs[-3:]
    J, I, K, M = here.shape
    shared = (here, before, speed, lev_lo, lev_hi, out)
    p, inner = (0, 1) if low else (J - 1, J - 2)

    def row(r, left, right):
        ends = halo[0, r - row0], here[inner, r]
        cell_row(shared, p, r, left, right, *ends)

    copies = []
    for n, at in enumerate(range(row0, row0 + length, BLOCK)):
        end = min(at + BLOCK, row0 + length)
        if at == 0:
            row(0, lon_lo[p], here[p, 1])

        @pl.loop(max(at, 1), min(end, I - 1))
        def _(r):
            row(r, here[p, r - 1], here[p, r + 1])

        if end == I:
            row(I - 1, here[p, I - 2], lon_hi[p])
        rows = pl.ds(at, end - at)
        copies.append(pltpu.make_async_copy(out.at[p, rows], result.at[p, rows], sems.at[n]))
        copies[-1].start()
    for copy in copies:
        copy.wait()


def inner_body(final, *refs):
    here, before, speed, lon_lo, lon_hi, lev_lo, lev_hi = refs[:7]
    refs = refs[7:]
    out = refs[0]
    J, I, K, M = here.shape
    shared = (here, before, speed, lev_lo, lev_hi, out)

    @pl.loop(1, J - 1)
    def _(p):
        cell_row(shared, p, 0, lon_lo[p], here[p, 1], here[p - 1, 0], here[p + 1, 0])

        @pl.loop(1, I - 1)
        def _(r):
            cell_row(shared, p, r, here[p, r - 1], here[p, r + 1], here[p - 1, r], here[p + 1, r])

        cell_row(shared, p, I - 1, here[p, I - 2], lon_hi[p], here[p - 1, I - 1], here[p + 1, I - 1])

    if final:
        inner = pl.ds(1, J - 2)
        copied([(out.at[inner], refs[1].at[inner])], refs[2])


def local(field_now, earlier, speed_square):
    J, I, K, M = shape = field_now.shape
    dtype = field_now.dtype
    cut = I // 2
    chunks = [(0, cut), (cut, I - cut)]
    block = pltpu.VMEM(shape, dtype)

    def exchange(faces):
        first, final, under, over = faces
        lon_lo, lon_hi = sent(final, "lon", True), sent(first, "lon", False)
        lev_lo, lev_hi = sent(over, "lev", True), sent(under, "lev", False)
        return [held(x) for x in (lon_lo, lon_hi, lev_lo, lev_hi)]

    lows, highs = [], []
    for c, (at, length) in enumerate(chunks):
        whole = c == len(chunks) - 1
        lat_chunk = pltpu.VMEM((1, length, K, M), dtype)
        shapes = [lat_chunk] * 2 + ([block] + face_shapes(shape, dtype) if whole else [])
        got = call(functools.partial(stage_body, at, length, whole), [far(field_now)], [ANY], shapes,
                   [VMEM] * len(shapes), length * K * M, f"stage_{at}",
                   scratch=[pltpu.SemaphoreType.DMA((3,))])
        highs.append(sent(got[0], "lat", False))
        lows.append(sent(got[1], "lat", True))
    field, faces = got[2], exchange(got[3:7])
    before, speed = call(load_body, [far(earlier), far(speed_square)], [ANY] * 2, [block] * 2, [VMEM] * 2,
                         J * I * K * M, "load", scratch=[pltpu.SemaphoreType.DMA((2,))])
    for step in range(STEPS - 1):
        next_lows, next_highs = [], []
        for c, (at, length) in enumerate(chunks):
            last = c == len(chunks) - 1
            operands = [held(field), held(before), held(speed), *faces, held(lows[c]), held(highs[c])]
            shapes = [block] + [pltpu.VMEM((1, length, K, M), dtype)] * 2
            if last:
                shapes += face_shapes(shape, dtype)
            got = call(functools.partial(edge_body, at, length, last), operands, [VMEM] * 9, shapes,
                       [VMEM] * len(shapes), 2 * length * K * M, f"edge_{step}_{at}", {1: 0})
            before = got[0]
            next_highs.append(sent(got[1], "lat", False))
            next_lows.append(sent(got[2], "lat", True))
            if last:
                next_faces = exchange(got[3:7])
            if c == 0:
                operands[1] = held(before)
                before, = call(functools.partial(inner_body, False), operands[:7], [VMEM] * 7, [block], [VMEM],
                               (J - 2) * I * K * M, f"inner_{step}", {1: 0})
        lows, highs, faces = next_lows, next_highs, next_faces
        before, field = field, before

    shapes = [block, jax.ShapeDtypeStruct(shape, dtype)]
    operands = [held(field), held(before), held(speed), *faces]
    before, result = call(functools.partial(inner_body, True), operands, [VMEM] * 7, shapes, [VMEM, ANY],
                          (J - 2) * I * K * M, "inner_final", {1: 0}, [pltpu.SemaphoreType.DMA((1,))])
    for c, (at, length) in enumerate(chunks):
        for low, halo in ((True, lows[c]), (False, highs[c])):
            operands = [held(field), held(before), held(speed), *faces, held(halo), result]
            before, result = call(
                functools.partial(final_body, at, length, low), operands, [VMEM] * 8 + [ANY], shapes, [VMEM, ANY],
                length * K * M, f"final_{at}_{int(low)}", {1: 0, 8: 1},
                [pltpu.SemaphoreType.DMA((-(-length // BLOCK),))])
    return result


def solution(mesh):
    spec = P("lat", "lon", "lev", None)
    return jax.shard_map(
        local,
        mesh=mesh,
        in_specs=(spec, spec, spec),
        out_specs=spec,
        check_vma=False,
    )
```
